256 devices in a mesh: rep: 1, dp: 256 (over x, y, z, core).
Axes of the slice: x: 4, y: 4, z: 8, core: 2. Of those that a mesh axis runs over, the one named last changes fastest.
Arguments:
- a: bfloat16 [256, 2, 2048, 1280], P(('rep', 'dp'))
- g: bfloat16 [256, 2, 2048, 3072], P(('rep', 'dp'))
Outputs:
- output: bfloat16 [2, 1280, 3072], P('rep')
All inputs are finite; a program needn't handle non-finite values.
Results may differ from the reference program's by a relative error of at most 0.012.
Values are sent between devices in bfloat16 or wider.
A program may use at most 768 MiB of HBM per device.

```python
import jax
import jax.numpy as jnp
from jax import lax

DEVICES = 256
MATRICES = 2
TOKENS = 2048
D = 1280
FF = 3072


def setup_inputs(seed: int = 0, part: int = 0) -> dict:
    ka, kg, ks = (jax.random.fold_in(k, part) for k in jax.random.split(jax.random.key(seed), 3))
    size = 2.0 ** jax.random.uniform(ks, (DEVICES, MATRICES, 1, 1), jnp.float32, -1.0, 1.0)
    a = jax.random.normal(ka, (DEVICES, MATRICES, TOKENS, D), jnp.float32)
    g = size * jax.random.normal(kg, (DEVICES, MATRICES, TOKENS, FF), jnp.float32) * (DEVICES * TOKENS) ** -0.5
    return {"a": a.astype(jnp.bfloat16), "g": g.astype(jnp.bfloat16)}


def reference(a, g):
    def take(so_far, one):
        term = jnp.einsum("ntd,ntf->ndf", *one, preferred_element_type=jnp.float32).astype(jnp.bfloat16)
        return so_far + term.astype(jnp.float32), None

    return lax.scan(take, jnp.zeros((MATRICES, D, FF), jnp.float32), (a, g))[0].astype(jnp.bfloat16)
```

```python
import functools

import jax
import jax.numpy as jnp
from jax import lax
from jax.experimental import pallas as pl
from jax.experimental.pallas import tpu as pltpu
from jax.sharding import PartitionSpec as P

MESH = pl.DeviceIdType.MESH
BF16, F32 = jnp.bfloat16, jnp.float32
NX, NY, NZ = 4, 4, 8
SIZE = {"x": NX, "y": NY, "z": NZ}
CHUNKS = 5
UNIT = 256
WIDE = 3072
COLOUR = 1024
TILE = 512
TILES = WIDE // TILE
ORDER = ("xyz", "yxz", "zxy")
SLOTS = 272
HOPS = 17


def pos(h):
    return 6 + 2 * h


def add(a, n, k):
    return lax.rem(a + (k + n), n)


class Box:
    def __init__(self, row, rows, col, cols):
        self.row, self.rows, self.col, self.cols = row, rows, col, cols

    def half(self, h):
        if self.rows >= 32:
            r = self.rows // 2
            return Box(self.row + r * h, r, self.col, self.cols)
        c = self.cols // 2
        return Box(self.row, self.rows, self.col + c * h, c)


def at(ref, base, colour, box):
    row = base + box.row
    col = COLOUR * colour + box.col
    if not isinstance(row, int):
        row = pl.multiple_of(row, 16)
    if not isinstance(col, int):
        col = pl.multiple_of(col, 128)
    return ref.at[pl.ds(row, box.rows), pl.ds(col, box.cols)]


def block(colour, level, i, within):
    w = within
    if colour < 2:
        if level == 0:
            return Box(64 * i, 64, 0, 1024)
        if level == 1:
            return Box(w.row + 16 * i, 16, 0, 1024)
        return Box(w.row, 16, 128 * i, 128)
    if level == 0:
        return Box(32 * i, 32, 0, 1024)
    if level == 1:
        return Box(w.row + 16 * (i // 2), 16, 512 * lax.rem(i, 2), 512)
    return Box(w.row, 16, w.col + 128 * i, 128)


def landing(colour, level, way, s):
    if level == 0:
        full = 64 if colour < 2 else 32
        m = 2 if colour < 2 else 4
        rows = full // 2 if s == 0 else full
        row = way * (full // 2 + full * (m - 1)) + (0 if s == 0 else full // 2 + full * (s - 1))
        return Box(row, rows, 0, 1024)
    if level == 1:
        if colour < 2:
            if s == 0:
                return Box(192, 16, 512 * way, 512)
            return Box(208 + 16 * way, 16, 0, 1024)
        if s == 0:
            return Box(224, 16, 256 * way, 256)
        return Box(224 + 16 * way, 16, 512 * (1 - way), 512)
    row = 240 if colour < 2 else 256
    if way == 0:
        return Box(row, 16, 128 * s, 128)
    return Box(row, 16, 512 + 128 * s, 128)


def rows_loop(rows, body):
    if rows == 16:
        body(0)
    else:

        def step(i, _):
            body(pl.multiple_of(i * 16, 16))
            return 0

        lax.fori_loop(0, rows // 16, step, 0)


def kernel(a, g, G, av, gv, X, F, R, a_sem, g_sem, in_send, in_recv, hop_recv, ici_send, out_send, out_recv):
    me = lax.axis_index("dp")
    core = lax.rem(me, 2)
    place = {"x": me // (NY * NZ * 2), "y": lax.rem(me // (NZ * 2), NY), "z": lax.rem(me // 2, NZ)}

    def device(p, c):
        return ((p["x"] * NY + p["y"]) * NZ + p["z"]) * 2 + c

    def beside(axis, k):
        return device({**place, axis: add(place[axis], SIZE[axis], k)}, core)

    up = {d: beside(d, 1) for d in "xyz"}
    down = {d: beside(d, -1) for d in "xyz"}
    partner = me + 1 - 2 * core

    barrier = pltpu.get_barrier_semaphore()
    for peer in (*up.values(), *down.values(), partner):
        pl.semaphore_signal(barrier, inc=1, device_id={"dp": peer}, device_id_type=MESH)
    pl.semaphore_wait(barrier, 7)

    ahead = {d: jnp.where(core == 0, up[d], down[d]) for d in "xyz"}
    behind = {d: jnp.where(core == 0, down[d], up[d]) for d in "xyz"}
    sign = 1 - 2 * core

    def own_base(c):
        return 2 * UNIT * c + UNIT * core

    def send(src, dst, colour, recv, peer):
        pltpu.make_async_remote_copy(
            src, dst, ici_send.at[colour], recv, device_id={"dp": peer}, device_id_type=MESH
        ).start()

    def arrived(box, times, sem):
        view = X.at[pl.ds(0, box.rows * times), pl.ds(0, box.cols)]
        pltpu.make_async_copy(view, view, sem).wait()

    def load_a(c, slot):
        copies = []
        for h in range(2):
            unit = 2 * c + (core if h == 0 else 1 - core)
            n = unit // 5
            col = pl.multiple_of(UNIT * (unit - 5 * n), UNIT)
            copies.append(
                pltpu.make_async_copy(
                    a.at[0, n, :, pl.ds(col, UNIT)], av.at[slot, :, pl.ds(UNIT * h, UNIT)], a_sem.at[slot, h]
                )
            )
        return copies

    def load_g(c, t, h):
        unit = 2 * c + (core if h == 0 else 1 - core)
        slot = 2 * h + t % 2
        return pltpu.make_async_copy(g.at[0, unit // 5, :, pl.ds(TILE * t, TILE)], gv.at[slot], g_sem.at[slot])

    def fetch(c, t):
        load_g(c, t, 0).start()

        @pl.when(c == 2)
        def _():
            load_g(c, t, 1).start()

    def matmul(c, t):
        if t == 0:
            for copy in load_a(c, lax.rem(c, 2)):
                copy.wait()

            @pl.when(c + 1 < CHUNKS)
            def _():
                for copy in load_a(c + 1, lax.rem(c + 1, 2)):
                    copy.start()

        if t < TILES - 1:
            fetch(c, t + 1)
        else:

            @pl.when(c + 1 < CHUNKS)
            def _():
                fetch(c + 1, 0)

        load_g(c, t, 0).wait()

        @pl.when(c == 2)
        def _():
            load_g(c, t, 1).wait()

        slot = lax.rem(c, 2)
        other = jnp.where(c == 2, 2 + t % 2, t % 2)
        rows = pl.ds(pl.multiple_of(UNIT * c, UNIT), UNIT)
        cols = pl.ds(TILE * t, TILE)
        dims = (((0,), (0,)), ((), ()))
        theirs = lax.dot_general(av[slot, :, UNIT:], gv[other], dims, preferred_element_type=F32)
        X[rows, cols] = theirs.astype(BF16)
        there = pl.ds(pl.multiple_of(2 * UNIT * c + UNIT * (1 - core), UNIT), UNIT)
        pltpu.make_async_remote_copy(
            X.at[rows, cols],
            G.at[there, cols],
            in_send.at[c],
            in_recv.at[c],
            device_id={"dp": partner},
            device_id_type=MESH,
        ).start()
        F[rows, cols] = lax.dot_general(av[slot, :, :UNIT], gv[t % 2], dims, preferred_element_type=F32)

    def hop_reduce(c, k, level, s, path):
        axis = ORDER[k][level]
        n = SIZE[axis]
        m = n // 2
        p = place[axis]
        whole = level == 2
        x_base, g_base, r_base = UNIT * c, own_base(c), SLOTS * c
        ups, downs, sg = (ahead, behind, sign) if whole else (up, down, 1)
        within = path[level - 1] if level else None

        def own(box, r):
            b = Box(box.row + r, 16, box.col, box.cols)
            value = at(F, x_base, k, b)[...]
            if level == 0:
                value = value + at(G, g_base, k, b)[...].astype(F32)
            return value

        def got(box, r):
            return at(R, r_base, k, Box(box.row + r, 16, box.col, box.cols))[...].astype(F32)

        def put(box, extra):
            def body(r):
                value = own(box, r)
                if extra is not None:
                    value = value + got(extra, r)
                at(X, x_base, k, Box(box.row + r, 16, box.col, box.cols))[...] = value.astype(BF16)

            rows_loop(box.rows, body)

        def go(box, way, step):
            peer = (ups if way == 0 else downs)[axis]
            send(at(X, x_base, k, box), at(R, r_base, k, landing(k, level, way, step)), k, recv(level, step + 1), peer)

        def recv(lv, step):
            first = {0: 1, 1: 1 + SIZE[ORDER[k][0]] // 2, 2: 1 + (SIZE[ORDER[k][0]] + SIZE[ORDER[k][1]]) // 2}[lv]
            return hop_recv.at[c, k, first + step - 1]

        def blk(o):
            return block(k, level, add(p, n, sg * o), within)

        if s > 0:
            one = blk(0)
            if s == 1:
                arrived(one, 1, recv(level, s))
            else:
                arrived(one, 2, recv(level, s))
        if s == 0:
            far = blk(m)
            if whole:
                put(far, None)
                go(far, 0, 0)
            else:
                for way in range(2):
                    put(far.half(way), None)
                    go(far.half(way), way, 0)
        elif s < m:
            for way in range(2):
                box = blk((m - s) if way == 0 else -(m - s))
                if s == 1 and whole:
                    put(box, landing(k, level, 0, 0) if way == 0 else None)
                elif s == 1:
                    put(box.half(way), landing(k, level, way, 0))
                    put(box.half(1 - way), None)
                else:
                    put(box, landing(k, level, way, s - 1))
                go(box, way, s)
        else:
            box = blk(0)
            first, second = landing(k, level, 0, m - 1), landing(k, level, 1, m - 1)

            def body(r):
                value = own(box, r) + got(first, r) + got(second, r)
                b = Box(box.row + r, 16, box.col, box.cols)
                if whole:
                    at(G, g_base, k, b)[...] = value.astype(BF16)
                else:
                    at(F, x_base, k, b)[...] = value

            rows_loop(box.rows, body)

    def hop_gather(c, k, level, s, path):
        axis = ORDER[k][level]
        n = SIZE[axis]
        m = n // 2
        p = place[axis]
        whole = level == 2
        g_base = own_base(c)
        ups, downs, sg = (ahead, behind, sign) if whole else (up, down, 1)
        within = path[level - 1] if level else None
        sizes = [SIZE[d] // 2 for d in ORDER[k]]
        first = {2: 1 + sum(sizes), 1: 1 + sum(sizes) + sizes[2], 0: 1 + sum(sizes) + sizes[2] + sizes[1]}[level]

        def recv(step):
            return hop_recv.at[c, k, first + step - 1]

        def blk(o):
            return block(k, level, add(p, n, sg * o), within)

        def go(box, way, step):
            peer = (ups if way == 0 else downs)[axis]
            view = at(G, g_base, k, box)
            send(view, view, k, recv(step + 1), peer)

        def across(box):
            if level == 0:
                view = at(G, g_base, k, box)
                pltpu.make_async_remote_copy(
                    view, view, out_send, out_recv, device_id={"dp": partner}, device_id_type=MESH
                ).start()

        if s == 0:
            go(blk(0), 0, 0)
            go(blk(0), 1, 0)
            across(blk(0))
            return
        arrived(blk(0), 2 if s < m else 1, recv(s))
        if s == m:
            across(blk(m))
            return
        from_below, from_above = blk(-s), blk(s)
        if s < m - 1:
            go(from_below, 0, s)
            go(from_above, 1, s)
        elif whole:
            go(from_below, 0, s)
        else:
            go(from_below.half(0), 0, s)
            go(from_above.half(1), 1, s)
        across(from_below)
        across(from_above)

    def plan(k):
        sizes = [SIZE[d] // 2 for d in ORDER[k]]
        steps = [[] for _ in range(HOPS)]
        h = 0
        for level in range(3):
            for s in range(sizes[level] + 1):
                steps[h].append((hop_reduce, level, s))
                h += s < sizes[level]
        for level in (2, 1, 0):
            for s in range(sizes[level] + 1):
                steps[h].append((hop_gather, level, s))
                h += s < sizes[level]
        assert h == HOPS - 1
        return steps

    plans = [plan(k) for k in range(3)]

    def hop(h, c):
        if h == 0:
            view = X.at[pl.ds(0, UNIT), :]
            pltpu.make_async_copy(view, view, in_recv.at[c]).wait()
            pltpu.make_async_copy(view, view, in_send.at[c]).wait()
        for k in (2, 0, 1):
            path = []
            for level in range(3):
                path.append(block(k, level, place[ORDER[k][level]], path[-1] if path else None))
            for f, level, s in plans[k][h]:
                f(c, k, level, s, path)

    for copy in load_a(0, 0):
        copy.start()
    fetch(jnp.int32(0), 0)

    where = [(pos(h) // 6, pos(h) % 6) for h in range(HOPS)]
    last = max(j for j, _ in where)

    def iteration(i, _):
        for q in range(6):
            pl.when(i < CHUNKS)(functools.partial(matmul, i, q))
            for h in reversed(range(HOPS)):
                j, at_q = where[h]
                if at_q == q:
                    c = i - j
                    pl.when(jnp.logical_and(c >= 0, c < CHUNKS))(functools.partial(hop, h, c))
        return 0

    lax.fori_loop(0, CHUNKS + last, iteration, 0)

    half = X.at[pl.ds(0, CHUNKS * UNIT), :]
    pltpu.make_async_copy(half, half, out_recv).wait()
    pltpu.make_async_copy(half, half, out_send).wait()
    for k in range(3):
        view = G.at[pl.ds(0, 2032), pl.ds(0, 1280)]
        pltpu.make_async_copy(view, view, ici_send.at[k]).wait()


def unload(v, o, sem):
    copy = pltpu.make_async_copy(v, o, sem)
    copy.start()
    copy.wait()


def solution(mesh):
    def body(a, g):
        dma = pltpu.SemaphoreType.DMA
        held = pl.pallas_call(
            kernel,
            out_shape=pltpu.VMEM((2 * CHUNKS * UNIT, WIDE), BF16),
            in_specs=[pl.BlockSpec(memory_space=pltpu.HBM)] * 2,
            out_specs=pl.BlockSpec(memory_space=pltpu.VMEM),
            scratch_shapes=[
                pltpu.VMEM((2, 2048, 2 * UNIT), BF16),
                pltpu.VMEM((4, 2048, TILE), BF16),
                pltpu.VMEM((CHUNKS * UNIT, WIDE), BF16),
                pltpu.VMEM((CHUNKS * UNIT, WIDE), F32),
                pltpu.VMEM((CHUNKS * SLOTS, WIDE), BF16),
                dma((2, 2)),
                dma((4,)),
                dma((CHUNKS,)),
                dma((CHUNKS,)),
                dma((CHUNKS, 3, HOPS)),
                dma((3,)),
                dma,
                dma,
            ],
            compiler_params=pltpu.CompilerParams(
                collective_id=0, has_side_effects=True, vmem_limit_bytes=50_000_000
            ),
            name="sums",
        )(a, g)
        out = pl.pallas_call(
            unload,
            out_shape=jax.ShapeDtypeStruct(held.shape, held.dtype),
            in_specs=[pl.BlockSpec(memory_space=pltpu.VMEM)],
            out_specs=pl.BlockSpec(memory_space=pltpu.HBM),
            scratch_shapes=[dma],
            compiler_params=pltpu.CompilerParams(vmem_limit_bytes=1 << 20),
            name="unload",
        )(held)
        return out.reshape(2, CHUNKS * UNIT, WIDE)

    spec = P(("rep", "dp"))
    return jax.shard_map(body, mesh=mesh, in_specs=(spec, spec), out_specs=P("rep"), check_vma=False)
```

```python
import functools

import jax
import jax.numpy as jnp
from jax import lax
from jax.experimental import pallas as pl
from jax.experimental.pallas import tpu as pltpu
from jax.sharding import PartitionSpec as P

MESH = pl.DeviceIdType.MESH
BF16, F32 = jnp.bfloat16, jnp.float32
NX, NY, NZ = 4, 4, 8
SIZE = {"x": NX, "y": NY, "z": NZ}
CHUNKS = 5
UNIT = 256
WIDE = 3072
COLOUR = 1024
TILE = 512
TILES = WIDE // TILE
ORDER = ("xyz", "yxz", "zxy")
SLOTS = 272
LOADS = 4
AHEAD = 2
DIRECT = ((2,), (2,), (1, 2))


def add(a, n, k):
    return lax.rem(a + (k + n), n)


class Box:
    def __init__(self, row, rows, col, cols):
        self.row, self.rows, self.col, self.cols = row, rows, col, cols

    def half(self, h):
        if self.rows >= 32:
            r = self.rows // 2
            return Box(self.row + r * h, r, self.col, self.cols)
        c = self.cols // 2
        return Box(self.row, self.rows, self.col + c * h, c)


def at(ref, base, colour, box):
    row = base + box.row
    col = COLOUR * colour + box.col
    if not isinstance(row, int):
        row = pl.multiple_of(row, 16)
    if not isinstance(col, int):
        col = pl.multiple_of(col, 128)
    return ref.at[pl.ds(row, box.rows), pl.ds(col, box.cols)]


def block(colour, level, i, within):
    w = within
    if colour < 2:
        if level == 0:
            return Box(64 * i, 64, 0, 1024)
        if level == 1:
            return Box(w.row + 16 * i, 16, 0, 1024)
        return Box(w.row, 16, 128 * i, 128)
    if level == 0:
        return Box(32 * i, 32, 0, 1024)
    if level == 1:
        return Box(w.row + 16 * (i // 2), 16, 512 * lax.rem(i, 2), 512)
    return Box(w.row, 16, w.col + 128 * i, 128)


def landing_direct(colour, level, o):
    o -= 1
    if level == 2:
        return Box(240 if colour < 2 else 256, 16, 128 * o, 128)
    if colour < 2:
        return Box(192 + 16 * o, 16, 0, 1024)
    return Box(224 + 16 * (o // 2), 16, 512 * (o % 2), 512)


def landing(colour, level, way, s):
    if level == 0:
        full = 64 if colour < 2 else 32
        m = 2 if colour < 2 else 4
        rows = full // 2 if s == 0 else full
        row = way * (full // 2 + full * (m - 1)) + (0 if s == 0 else full // 2 + full * (s - 1))
        return Box(row, rows, 0, 1024)
    if level == 1:
        if colour < 2:
            if s == 0:
                return Box(192, 16, 512 * way, 512)
            return Box(208 + 16 * way, 16, 0, 1024)
        if s == 0:
            return Box(224, 16, 256 * way, 256)
        return Box(224 + 16 * way, 16, 512 * (1 - way), 512)
    row = 240 if colour < 2 else 256
    if way == 0:
        return Box(row, 16, 128 * s, 128)
    return Box(row, 16, 512 + 128 * s, 128)


FIRST = (-1, 3, 5, 9, 13, 15)


def plan(k, direct):
    hops = [[]]
    for gather, levels in ((False, (0, 1, 2)), (True, (2, 1, 0))):
        for level in levels:
            steps = 1 if level in direct else SIZE[ORDER[k][level]] // 2
            for s in range(steps + 1):
                hops[-1].append((gather, level, s))
                if s < steps:
                    hops.append([])
    return hops


def messages(k, gather, level, s):
    axis = ORDER[k][level]
    n = SIZE[axis]
    m = n // 2
    full = UNIT * COLOUR * 2
    for j in range(level + 1):
        full //= SIZE[ORDER[k][j]]
    if level in DIRECT[k]:
        far = 0.75 * (m - 1)
        return [(axis, 0, full * m * (m + 1) // 2, far), (axis, 1, full * m * (m - 1) // 2, far)] if s == 0 else []
    if s == m:
        return []
    if s == (m - 1 if gather else 0):
        full //= 2
    return [(axis, 0, full, 0), (axis, 1, full, 0)]


def sequence():
    latency, rate, tile_time, hop_time = 2.3, 46.6e3, 1.5, 0.035
    plans = [plan(k, DIRECT[k]) for k in range(3)]
    free, arrival, order = {}, {}, []
    now, tile = 3.5, 0
    while True:
        waiting = [x for x in arrival if arrival[x] is not None and x not in order]
        ready = [x for x in waiting if arrival[x] <= now]
        if ready:
            c, k, h = x = min(ready, key=lambda x: (arrival[x] + 2 * x[0], x))
            order.append(x)
            spent = hop_time + 0.1 * (h == 0)
            for gather, level, s in plans[k][h]:
                spent += 0.08 * (level == 0 and not gather)
                for axis, way, size, extra in messages(k, gather, level, s):
                    end = max(now + spent, free.get((axis, way), 0)) + size / rate
                    free[axis, way] = end
                    to = c, k, h + 1
                    arrival[to] = max(arrival.get(to, 0), end + latency + extra)
            now += spent
        elif tile < CHUNKS * TILES:
            order.append(None)
            now += tile_time
            tile += 1
            if tile % (TILES // 3) == 0:
                arrival[(tile - 1) // TILES, (tile - 1) % TILES // (TILES // 3), 0] = now + 1.8
        elif waiting:
            now = min(arrival[x] for x in waiting)
        else:
            return order


def rows_loop(rows, body):
    if rows == 16:
        body(0)
    else:

        def step(i, _):
            body(pl.multiple_of(i * 16, 16))
            return 0

        lax.fori_loop(0, rows // 16, step, 0)


def kernel(a, g, G, av, gv, X, F, R, a_sem, g_sem, in_send, in_recv, hop_recv, ici_send, out_send, out_recv):
    me = lax.axis_index("dp")
    core = lax.rem(me, 2)
    place = {"x": me // (NY * NZ * 2), "y": lax.rem(me // (NZ * 2), NY), "z": lax.rem(me // 2, NZ)}

    def device(p, c):
        return ((p["x"] * NY + p["y"]) * NZ + p["z"]) * 2 + c

    def beside(axis, k):
        return device({**place, axis: add(place[axis], SIZE[axis], k)}, core)

    up = {d: beside(d, 1) for d in "xyz"}
    down = {d: beside(d, -1) for d in "xyz"}
    partner = me + 1 - 2 * core

    def load_a(c, slot):
        copies = []
        for h in range(2):
            unit = 2 * c + (core if h == 0 else 1 - core)
            n = unit // 5
            col = pl.multiple_of(UNIT * (unit - 5 * n), UNIT)
            copies.append(
                pltpu.make_async_copy(
                    a.at[0, n, :, pl.ds(col, UNIT)], av.at[slot, :, pl.ds(UNIT * h, UNIT)], a_sem.at[slot, h]
                )
            )
        return copies

    def place_g(i, h):
        return lax.rem(i, AHEAD) + AHEAD * h

    def load_g(i, h):
        c = i // TILES
        unit = 2 * c + (core if h == 0 else 1 - core)
        slot = place_g(i, h)
        cols = pl.ds(pl.multiple_of(TILE * (i - TILES * c), TILE), TILE)
        return pltpu.make_async_copy(g.at[0, unit // 5, :, cols], gv.at[slot], g_sem.at[slot])

    def fetch(i):
        load_g(i, 0).start()

        @pl.when(i // TILES == 2)
        def _():
            load_g(i, 1).start()

    for copy in load_a(0, 0):
        copy.start()
    for i in range(AHEAD - 1):
        fetch(jnp.int32(i))

    peers = [beside(d, o) for d in "xyz" for o in range(1, SIZE[d])] + [partner]
    barrier = pltpu.get_barrier_semaphore()
    for peer in peers:
        pl.semaphore_signal(barrier, inc=1, device_id={"dp": peer}, device_id_type=MESH)
    ahead = {d: jnp.where(core == 0, up[d], down[d]) for d in "xyz"}
    behind = {d: jnp.where(core == 0, down[d], up[d]) for d in "xyz"}
    sign = 1 - 2 * core

    def own_base(c):
        return 2 * UNIT * c + UNIT * core

    def send(src, dst, colour, recv, peer):
        pltpu.make_async_remote_copy(
            src, dst, ici_send.at[colour], recv, device_id={"dp": peer}, device_id_type=MESH
        ).start()

    def arrived(box, times, sem):
        view = X.at[pl.ds(0, box.rows * times), pl.ds(0, box.cols)]
        pltpu.make_async_copy(view, view, sem).wait()

    def matmul(i, first=False):
        c = i // TILES
        q = i - TILES * c
        slot = lax.rem(c, 2)

        @pl.when(q == 0)
        def _():
            for copy in load_a(c, slot):
                copy.wait()

            @pl.when(c + 1 < CHUNKS)
            def _():
                for copy in load_a(c + 1, 1 - slot):
                    copy.start()

        @pl.when(i + AHEAD - 1 < CHUNKS * TILES)
        def _():
            fetch(i + AHEAD - 1)

        load_g(i, 0).wait()

        @pl.when(c == 2)
        def _():
            load_g(i, 1).wait()

        mine = place_g(i, 0)
        other = mine + jnp.where(c == 2, AHEAD, 0)
        rows = pl.ds(pl.multiple_of(UNIT * c, UNIT), UNIT)
        cols = pl.ds(pl.multiple_of(TILE * q, TILE), TILE)
        dims = (((0,), (0,)), ((), ()))
        theirs = lax.dot_general(av[slot, :, UNIT:], gv[other], dims, preferred_element_type=F32)
        X[rows, cols] = theirs.astype(BF16)
        if first:
            pl.semaphore_wait(barrier, len(peers))
        there = pl.ds(pl.multiple_of(2 * UNIT * c + UNIT * (1 - core), UNIT), UNIT)
        k = q // (TILES // 3)
        pltpu.make_async_remote_copy(
            X.at[rows, cols],
            G.at[there, cols],
            in_send.at[c, k],
            in_recv.at[c, k],
            device_id={"dp": partner},
            device_id_type=MESH,
        ).start()
        F[rows, cols] = lax.dot_general(av[slot, :, :UNIT], gv[mine], dims, preferred_element_type=F32)

    def hop_reduce(c, k, level, s, path):
        axis = ORDER[k][level]
        n = SIZE[axis]
        m = n // 2
        p = place[axis]
        whole = level == 2
        x_base, g_base, r_base = UNIT * c, own_base(c), SLOTS * c
        ups, downs, sg = (ahead, behind, sign) if whole else (up, down, 1)
        within = path[level - 1] if level else None

        def own(box, r):
            b = Box(box.row + r, 16, box.col, box.cols)
            value = at(F, x_base, k, b)[...]
            if level == 0:
                value = value + at(G, g_base, k, b)[...].astype(F32)
            return value

        def got(box, r):
            return at(R, r_base, k, Box(box.row + r, 16, box.col, box.cols))[...].astype(F32)

        def put(box, extra):
            def body(r):
                value = own(box, r)
                if extra is not None:
                    value = value + got(extra, r)
                at(X, x_base, k, Box(box.row + r, 16, box.col, box.cols))[...] = value.astype(BF16)

            rows_loop(box.rows, body)

        def go(box, way, step):
            peer = (ups if way == 0 else downs)[axis]
            send(at(X, x_base, k, box), at(R, r_base, k, landing(k, level, way, step)), k, recv(level, step + 1), peer)

        def recv(lv, step):
            return hop_recv.at[c, k, FIRST[lv] + step]

        def blk(o):
            return block(k, level, add(p, n, sg * o), within)

        if level in DIRECT[k]:
            if s == 0:
                for o in range(1, n):
                    box = block(k, level, add(p, n, o), within)
                    put(box, None)
                    send(
                        at(X, x_base, k, box),
                        at(R, r_base, k, landing_direct(k, level, o)),
                        k,
                        recv(level, 1),
                        beside(axis, o),
                    )
            else:
                box = blk(0)
                arrived(box, n - 1, recv(level, 1))

                def body(r):
                    value = own(box, r)
                    for o in range(1, n):
                        value = value + got(landing_direct(k, level, o), r)
                    if whole:
                        at(G, g_base, k, box)[...] = value.astype(BF16)
                    else:
                        at(F, x_base, k, box)[...] = value

                rows_loop(box.rows, body)
            return

        if s > 0:
            one = blk(0)
            if s == 1:
                arrived(one, 1, recv(level, s))
            else:
                arrived(one, 2, recv(level, s))
        if s == 0:
            far = blk(m)
            if whole:
                put(far, None)
                go(far, 0, 0)
            else:
                for way in range(2):
                    put(far.half(way), None)
                    go(far.half(way), way, 0)
        elif s < m:
            for way in range(2):
                box = blk((m - s) if way == 0 else -(m - s))
                if s == 1 and whole:
                    put(box, landing(k, level, 0, 0) if way == 0 else None)
                elif s == 1:
                    put(box.half(way), landing(k, level, way, 0))
                    put(box.half(1 - way), None)
                else:
                    put(box, landing(k, level, way, s - 1))
                go(box, way, s)
        else:
            box = blk(0)
            first, second = landing(k, level, 0, m - 1), landing(k, level, 1, m - 1)

            def body(r):
                value = own(box, r) + got(first, r) + got(second, r)
                b = Box(box.row + r, 16, box.col, box.cols)
                if whole:
                    at(G, g_base, k, b)[...] = value.astype(BF16)
                else:
                    at(F, x_base, k, b)[...] = value

            rows_loop(box.rows, body)

    def hop_gather(c, k, level, s, path):
        axis = ORDER[k][level]
        n = SIZE[axis]
        m = n // 2
        p = place[axis]
        whole = level == 2
        g_base = own_base(c)
        ups, downs, sg = (ahead, behind, sign) if whole else (up, down, 1)
        within = path[level - 1] if level else None

        def recv(step):
            return hop_recv.at[c, k, FIRST[level + 3] + step]

        def blk(o):
            return block(k, level, add(p, n, sg * o), within)

        def go(box, way, step):
            peer = (ups if way == 0 else downs)[axis]
            view = at(G, g_base, k, box)
            send(view, view, k, recv(step + 1), peer)

        def across(box):
            if level == 0:
                view = at(G, g_base, k, box)
                pltpu.make_async_remote_copy(
                    view, view, out_send, out_recv, device_id={"dp": partner}, device_id_type=MESH
                ).start()

        if level in DIRECT[k]:
            if s == 0:
                view = at(G, g_base, k, blk(0))
                for o in range(1, n):
                    send(view, view, k, recv(1), beside(axis, o))
            else:
                arrived(blk(0), n - 1, recv(1))
            return
        if s == 0:
            go(blk(0), 0, 0)
            go(blk(0), 1, 0)
            across(blk(0))
            return
        arrived(blk(0), 2 if s < m else 1, recv(s))
        if s == m:
            across(blk(m))
            return
        from_below, from_above = blk(-s), blk(s)
        if s < m - 1:
            go(from_below, 0, s)
            go(from_above, 1, s)
        elif whole:
            go(from_below, 0, s)
        else:
            go(from_below.half(0), 0, s)
            go(from_above.half(1), 1, s)
        across(from_below)
        across(from_above)

    def hop(c, k, h):
        if h == 0:
            view = X.at[pl.ds(0, UNIT), pl.ds(0, COLOUR)]
            pltpu.make_async_copy(view, view, in_recv.at[c, k]).wait()
            pltpu.make_async_copy(view, view, in_send.at[c, k]).wait()
        path = []
        for level in range(3):
            path.append(block(k, level, place[ORDER[k][level]], path[-1] if path else None))
        for gather, level, s in plan(k, DIRECT[k])[h]:
            (hop_gather if gather else hop_reduce)(c, k, level, s, path)

    after = {}
    tile = -1
    for item in sequence():
        if item is None:
            tile += 1
        else:
            after.setdefault(tile, []).append(item)
    tiles = CHUNKS * TILES
    assert tile == tiles - 1 and min(after) > 0

    def run(hops):
        for c, k, h in hops:
            hop(c, k, h)

    def step(i, _):
        matmul(i)
        for c in range(CHUNKS):
            mine = [j for j in after if j // TILES == c and j < tiles - 1]

            def of_chunk(mine=mine):
                for j in mine:
                    pl.when(i == j)(functools.partial(run, after[j]))

            if mine:
                pl.when(i // TILES == c)(of_chunk)
        return 0

    matmul(jnp.int32(0), first=True)
    lax.fori_loop(1, tiles, step, 0)
    run(after[tiles - 1])

    half = X.at[pl.ds(0, CHUNKS * UNIT), :]
    pltpu.make_async_copy(half, half, out_recv).wait()
    pltpu.make_async_copy(half, half, out_send).wait()
    for k in range(3):
        view = G.at[pl.ds(0, 2032), pl.ds(0, 1280)]
        pltpu.make_async_copy(view, view, ici_send.at[k]).wait()


def unload(v, o, sem):
    copy = pltpu.make_async_copy(v, o, sem)
    copy.start()
    copy.wait()


def solution(mesh):
    def body(a, g):
        dma = pltpu.SemaphoreType.DMA
        held = pl.pallas_call(
            kernel,
            out_shape=pltpu.VMEM((2 * CHUNKS * UNIT, WIDE), BF16),
            in_specs=[pl.BlockSpec(memory_space=pltpu.HBM)] * 2,
            out_specs=pl.BlockSpec(memory_space=pltpu.VMEM),
            scratch_shapes=[
                pltpu.VMEM((2, 2048, 2 * UNIT), BF16),
                pltpu.VMEM((LOADS, 2048, TILE), BF16),
                pltpu.VMEM((CHUNKS * UNIT, WIDE), BF16),
                pltpu.VMEM((CHUNKS * UNIT, WIDE), F32),
                pltpu.VMEM((CHUNKS * SLOTS, WIDE), BF16),
                dma((2, 2)),
                dma((LOADS,)),
                dma((CHUNKS, 3)),
                dma((CHUNKS, 3)),
                dma((CHUNKS, 3, 20)),
                dma((3,)),
                dma,
                dma,
            ],
            compiler_params=pltpu.CompilerParams(
                collective_id=0, has_side_effects=True, vmem_limit_bytes=50_000_000
            ),
            name="sums",
        )(a, g)
        out = pl.pallas_call(
            unload,
            out_shape=jax.ShapeDtypeStruct(held.shape, held.dtype),
            in_specs=[pl.BlockSpec(memory_space=pltpu.VMEM)],
            out_specs=pl.BlockSpec(memory_space=pltpu.HBM),
            scratch_shapes=[dma],
            compiler_params=pltpu.CompilerParams(vmem_limit_bytes=1 << 20),
            name="unload",
        )(held)
        return out.reshape(2, CHUNKS * UNIT, WIDE)

    spec = P(("rep", "dp"))
    return jax.shard_map(body, mesh=mesh, in_specs=(spec, spec), out_specs=P("rep"), check_vma=False)
```

```python
import functools

import jax
import jax.numpy as jnp
from jax import lax
from jax.experimental import pallas as pl
from jax.experimental.pallas import tpu as pltpu
from jax.sharding import PartitionSpec as P

MESH = pl.DeviceIdType.MESH
BF16, F32 = jnp.bfloat16, jnp.float32
NX, NY, NZ = 4, 4, 8
SIZE = {"x": NX, "y": NY, "z": NZ}
CHUNKS = 5
UNIT = 256
WIDE = 3072
COLOUR = 1024
TILE = 512
TILES = WIDE // TILE
ORDER = ("xyz", "yxz", "zxy")
SLOTS = 272
LOADS = 4
AHEAD = 2
PARTS = 8
DIRECT = ((2,), (2,), (1, 2))


def add(a, n, k):
    return lax.rem(a + (k + n), n)


class Box:
    def __init__(self, row, rows, col, cols):
        self.row, self.rows, self.col, self.cols = row, rows, col, cols

    def half(self, h):
        if self.rows >= 32:
            r = self.rows // 2
            return Box(self.row + r * h, r, self.col, self.cols)
        c = self.cols // 2
        return Box(self.row, self.rows, self.col + c * h, c)


def at(ref, base, colour, box):
    row = base + box.row
    col = COLOUR * colour + box.col
    if not isinstance(row, int):
        row = pl.multiple_of(row, 16)
    if not isinstance(col, int):
        col = pl.multiple_of(col, 128)
    return ref.at[pl.ds(row, box.rows), pl.ds(col, box.cols)]


def block(colour, level, i, within):
    w = within
    if colour < 2:
        if level == 0:
            return Box(64 * i, 64, 0, 1024)
        if level == 1:
            return Box(w.row + 16 * i, 16, 0, 1024)
        return Box(w.row, 16, 128 * i, 128)
    if level == 0:
        return Box(32 * i, 32, 0, 1024)
    if level == 1:
        return Box(w.row + 16 * (i // 2), 16, 512 * lax.rem(i, 2), 512)
    return Box(w.row, 16, w.col + 128 * i, 128)


def landing_direct(colour, level, o):
    o -= 1
    if level == 2:
        return Box(240 if colour < 2 else 256, 16, 128 * o, 128)
    if colour < 2:
        return Box(192 + 16 * o, 16, 0, 1024)
    return Box(224 + 16 * (o // 2), 16, 512 * (o % 2), 512)


def landing(colour, level, way, s):
    if level == 0:
        full = 64 if colour < 2 else 32
        m = 2 if colour < 2 else 4
        rows = full // 2 if s == 0 else full
        row = way * (full // 2 + full * (m - 1)) + (0 if s == 0 else full // 2 + full * (s - 1))
        return Box(row, rows, 0, 1024)
    if level == 1:
        if colour < 2:
            if s == 0:
                return Box(192, 16, 512 * way, 512)
            return Box(208 + 16 * way, 16, 0, 1024)
        if s == 0:
            return Box(224, 16, 256 * way, 256)
        return Box(224 + 16 * way, 16, 512 * (1 - way), 512)
    row = 240 if colour < 2 else 256
    if way == 0:
        return Box(row, 16, 128 * s, 128)
    return Box(row, 16, 512 + 128 * s, 128)


FIRST = (-1, 3, 5, 9, 13, 15)


def plan(k, direct):
    hops = [[]]
    for gather, levels in ((False, (0, 1, 2)), (True, (2, 1, 0))):
        for level in levels:
            steps = 1 if level in direct else SIZE[ORDER[k][level]] // 2
            for s in range(steps + 1):
                hops[-1].append((gather, level, s))
                if s < steps:
                    hops.append([])
    return hops


def messages(k, gather, level, s):
    axis = ORDER[k][level]
    n = SIZE[axis]
    m = n // 2
    full = UNIT * COLOUR * 2
    for j in range(level + 1):
        full //= SIZE[ORDER[k][j]]
    if level in DIRECT[k]:
        far = 0.75 * (m - 1)
        return [(axis, 0, full * m * (m + 1) // 2, far), (axis, 1, full * m * (m - 1) // 2, far)] if s == 0 else []
    if s == m:
        return []
    if s == (m - 1 if gather else 0):
        full //= 2
    return [(axis, 0, full, 0), (axis, 1, full, 0)]


def sequence():
    latency, rate, tile_time, hop_time = 2.3, 46.6e3, 1.55, 0.035
    plans = [plan(k, DIRECT[k]) for k in range(3)]
    free, arrival, order = {}, {}, []
    now, tile = 4.7, 0
    while True:
        waiting = [x for x in arrival if arrival[x] is not None and x not in order]
        ready = [x for x in waiting if arrival[x] <= now]
        if ready:
            c, k, h = x = min(ready, key=lambda x: (arrival[x] + 2 * x[0], x))
            order.append(x)
            spent = hop_time + 0.1 * (h == 0)
            for gather, level, s in plans[k][h]:
                spent += 0.08 * (level == 0 and not gather)
                for axis, way, size, extra in messages(k, gather, level, s):
                    end = max(now + spent, free.get((axis, way), 0)) + size / rate
                    free[axis, way] = end
                    to = c, k, h + 1
                    arrival[to] = max(arrival.get(to, 0), end + latency + extra)
            now += spent
        elif tile < CHUNKS * TILES:
            order.append(None)
            now += tile_time
            tile += 1
            if tile % (TILES // 3) == 0:
                arrival[(tile - 1) // TILES, ((tile - 1) % TILES // (TILES // 3) + 2) % 3, 0] = now + 1.8
        elif waiting:
            now = min(arrival[x] for x in waiting)
        else:
            return order


def rows_loop(rows, body):
    if rows == 16:
        body(0)
    else:

        def step(i, _):
            body(pl.multiple_of(i * 16, 16))
            return 0

        lax.fori_loop(0, rows // 16, step, 0)


def kernel(a, g, G, av, gv, X, F, R, a_sem, g_sem, in_send, in_recv, hop_recv, ici_send, out_send, out_recv):
    me = lax.axis_index("dp")
    core = lax.rem(me, 2)
    place = {"x": me // (NY * NZ * 2), "y": lax.rem(me // (NZ * 2), NY), "z": lax.rem(me // 2, NZ)}

    def device(p, c):
        return ((p["x"] * NY + p["y"]) * NZ + p["z"]) * 2 + c

    def beside(axis, k):
        return device({**place, axis: add(place[axis], SIZE[axis], k)}, core)

    up = {d: beside(d, 1) for d in "xyz"}
    down = {d: beside(d, -1) for d in "xyz"}
    partner = me + 1 - 2 * core

    def load_a(c, slot):
        copies = []
        for h in range(2):
            unit = 2 * c + (core if h == 0 else 1 - core)
            n = unit // 5
            col = pl.multiple_of(UNIT * (unit - 5 * n), UNIT)
            copies.append(
                pltpu.make_async_copy(
                    a.at[0, n, :, pl.ds(col, UNIT)], av.at[slot, :, pl.ds(UNIT * h, UNIT)], a_sem.at[slot, h]
                )
            )
        return copies

    def columns(q):
        return lax.rem(q + TILES // 3 * 2, TILES)

    def place_g(i, h):
        return lax.rem(i, AHEAD) + AHEAD * h

    def load_g(i, h):
        c = i // TILES
        unit = 2 * c + (core if h == 0 else 1 - core)
        slot = place_g(i, h)
        cols = pl.ds(pl.multiple_of(TILE * columns(i - TILES * c), TILE), TILE)
        return pltpu.make_async_copy(g.at[0, unit // 5, :, cols], gv.at[slot], g_sem.at[slot])

    def fetch(i):
        load_g(i, 0).start()

        @pl.when(i // TILES == 2)
        def _():
            load_g(i, 1).start()

    for copy in load_a(0, 0):
        copy.start()
    for i in range(AHEAD - 1):
        fetch(jnp.int32(i))

    peers = [beside(d, o) for d in "xyz" for o in range(1, SIZE[d])] + [partner]
    barrier = pltpu.get_barrier_semaphore()
    for peer in peers:
        pl.semaphore_signal(barrier, inc=1, device_id={"dp": peer}, device_id_type=MESH)
    ahead = {d: jnp.where(core == 0, up[d], down[d]) for d in "xyz"}
    behind = {d: jnp.where(core == 0, down[d], up[d]) for d in "xyz"}
    sign = 1 - 2 * core

    def own_base(c):
        return 2 * UNIT * c + UNIT * core

    def send(src, dst, colour, recv, peer):
        pltpu.make_async_remote_copy(
            src, dst, ici_send.at[colour], recv, device_id={"dp": peer}, device_id_type=MESH
        ).start()

    def arrived(box, times, sem):
        view = X.at[pl.ds(0, box.rows * times), pl.ds(0, box.cols)]
        pltpu.make_async_copy(view, view, sem).wait()

    def matmul(i, first=False):
        c = i // TILES
        q = i - TILES * c
        slot = lax.rem(c, 2)

        @pl.when(q == 0)
        def _():
            for copy in load_a(c, slot):
                copy.wait()

            @pl.when(c + 1 < CHUNKS)
            def _():
                for copy in load_a(c + 1, 1 - slot):
                    copy.start()

        @pl.when(i + AHEAD - 1 < CHUNKS * TILES)
        def _():
            fetch(i + AHEAD - 1)

        load_g(i, 0).wait()

        @pl.when(c == 2)
        def _():
            load_g(i, 1).wait()

        mine = place_g(i, 0)
        other = mine + jnp.where(c == 2, AHEAD, 0)
        rows = pl.ds(pl.multiple_of(UNIT * c, UNIT), UNIT)
        q = columns(q)
        cols = pl.ds(pl.multiple_of(TILE * q, TILE), TILE)
        dims = (((0,), (0,)), ((), ()))
        theirs = lax.dot_general(av[slot, :, UNIT:], gv[other], dims, preferred_element_type=F32)
        X[rows, cols] = theirs.astype(BF16)
        if first:
            pl.semaphore_wait(barrier, len(peers))
        there = pl.ds(pl.multiple_of(2 * UNIT * c + UNIT * (1 - core), UNIT), UNIT)
        k = q // (TILES // 3)
        pltpu.make_async_remote_copy(
            X.at[rows, cols],
            G.at[there, cols],
            in_send.at[c, k],
            in_recv.at[c, k],
            device_id={"dp": partner},
            device_id_type=MESH,
        ).start()
        F[rows, cols] = lax.dot_general(av[slot, :, :UNIT], gv[mine], dims, preferred_element_type=F32)

    def hop_reduce(c, k, level, s, path):
        axis = ORDER[k][level]
        n = SIZE[axis]
        m = n // 2
        p = place[axis]
        whole = level == 2
        x_base, g_base, r_base = UNIT * c, own_base(c), SLOTS * c
        ups, downs, sg = (ahead, behind, sign) if whole else (up, down, 1)
        within = path[level - 1] if level else None

        def own(box, r):
            b = Box(box.row + r, 16, box.col, box.cols)
            value = at(F, x_base, k, b)[...]
            if level == 0:
                value = value + at(G, g_base, k, b)[...].astype(F32)
            return value

        def got(box, r):
            return at(R, r_base, k, Box(box.row + r, 16, box.col, box.cols))[...].astype(F32)

        def put(box, extra):
            def body(r):
                value = own(box, r)
                if extra is not None:
                    value = value + got(extra, r)
                at(X, x_base, k, Box(box.row + r, 16, box.col, box.cols))[...] = value.astype(BF16)

            rows_loop(box.rows, body)

        def go(box, way, step):
            peer = (ups if way == 0 else downs)[axis]
            send(at(X, x_base, k, box), at(R, r_base, k, landing(k, level, way, step)), k, recv(level, step + 1), peer)

        def recv(lv, step):
            return hop_recv.at[c, k, FIRST[lv] + step]

        def blk(o):
            return block(k, level, add(p, n, sg * o), within)

        if level in DIRECT[k]:
            if s == 0:
                for o in range(1, n):
                    box = block(k, level, add(p, n, o), within)
                    put(box, None)
                    send(
                        at(X, x_base, k, box),
                        at(R, r_base, k, landing_direct(k, level, o)),
                        k,
                        recv(level, 1),
                        beside(axis, o),
                    )
            else:
                box = blk(0)
                arrived(box, n - 1, recv(level, 1))

                def body(r):
                    value = own(box, r)
                    for o in range(1, n):
                        value = value + got(landing_direct(k, level, o), r)
                    if whole:
                        at(G, g_base, k, box)[...] = value.astype(BF16)
                    else:
                        at(F, x_base, k, box)[...] = value

                rows_loop(box.rows, body)
            return

        if s > 0:
            one = blk(0)
            if s == 1:
                arrived(one, 1, recv(level, s))
            else:
                arrived(one, 2, recv(level, s))
        if s == 0:
            far = blk(m)
            if whole:
                put(far, None)
                go(far, 0, 0)
            else:
                for way in range(2):
                    put(far.half(way), None)
                    go(far.half(way), way, 0)
        elif s < m:
            for way in range(2):
                box = blk((m - s) if way == 0 else -(m - s))
                if s == 1 and whole:
                    put(box, landing(k, level, 0, 0) if way == 0 else None)
                elif s == 1:
                    put(box.half(way), landing(k, level, way, 0))
                    put(box.half(1 - way), None)
                else:
                    put(box, landing(k, level, way, s - 1))
                go(box, way, s)
        else:
            box = blk(0)
            first, second = landing(k, level, 0, m - 1), landing(k, level, 1, m - 1)

            def body(r):
                value = own(box, r) + got(first, r) + got(second, r)
                b = Box(box.row + r, 16, box.col, box.cols)
                if whole:
                    at(G, g_base, k, b)[...] = value.astype(BF16)
                else:
                    at(F, x_base, k, b)[...] = value

            rows_loop(box.rows, body)

    def hop_gather(c, k, level, s, path):
        axis = ORDER[k][level]
        n = SIZE[axis]
        m = n // 2
        p = place[axis]
        whole = level == 2
        g_base = own_base(c)
        ups, downs, sg = (ahead, behind, sign) if whole else (up, down, 1)
        within = path[level - 1] if level else None

        def recv(step):
            return hop_recv.at[c, k, FIRST[level + 3] + step]

        def blk(o):
            return block(k, level, add(p, n, sg * o), within)

        def go(box, way, step):
            peer = (ups if way == 0 else downs)[axis]
            view = at(G, g_base, k, box)
            send(view, view, k, recv(step + 1), peer)

        def across(box):
            if level == 0:
                view = at(G, g_base, k, box)
                pltpu.make_async_remote_copy(
                    view, view, out_send, out_recv, device_id={"dp": partner}, device_id_type=MESH
                ).start()

        if level in DIRECT[k]:
            if s == 0:
                view = at(G, g_base, k, blk(0))
                for o in range(1, n):
                    send(view, view, k, recv(1), beside(axis, o))
            else:
                arrived(blk(0), n - 1, recv(1))
            return
        if s == 0:
            go(blk(0), 0, 0)
            go(blk(0), 1, 0)
            across(blk(0))
            return
        arrived(blk(0), 2 if s < m else 1, recv(s))
        if s == m:
            across(blk(m))
            return
        from_below, from_above = blk(-s), blk(s)
        if s < m - 1:
            go(from_below, 0, s)
            go(from_above, 1, s)
        elif whole:
            go(from_below, 0, s)
        else:
            go(from_below.half(0), 0, s)
            go(from_above.half(1), 1, s)
        across(from_below)
        across(from_above)

    def hop(c, k, h):
        if h == 0:
            view = X.at[pl.ds(0, UNIT), pl.ds(0, COLOUR)]
            pltpu.make_async_copy(view, view, in_recv.at[c, k]).wait()
            pltpu.make_async_copy(view, view, in_send.at[c, k]).wait()
        path = []
        for level in range(3):
            path.append(block(k, level, place[ORDER[k][level]], path[-1] if path else None))
        for gather, level, s in plan(k, DIRECT[k])[h]:
            (hop_gather if gather else hop_reduce)(c, k, level, s, path)

    after = {}
    tile = -1
    for item in sequence():
        if item is None:
            tile += 1
        else:
            after.setdefault(tile, []).append(item)
    tiles = CHUNKS * TILES
    assert tile == tiles - 1 and min(after) > 0

    def run(hops):
        for c, k, h in hops:
            hop(c, k, h)

    def step(i, _):
        matmul(i)
        for c in range(CHUNKS):
            mine = [j for j in after if j // TILES == c and j < tiles - 1]

            def of_chunk(mine=mine):
                for j in mine:
                    pl.when(i == j)(functools.partial(run, after[j]))

            if mine:
                pl.when(i // TILES == c)(of_chunk)
        return 0

    matmul(jnp.int32(0), first=True)
    lax.fori_loop(1, tiles, step, 0)
    run(after[tiles - 1])

    half = X.at[pl.ds(0, CHUNKS * UNIT), :]
    pltpu.make_async_copy(half, half, out_recv).wait()
    pltpu.make_async_copy(half, half, out_send).wait()
    for k in range(3):
        view = G.at[pl.ds(0, 2032), pl.ds(0, 1280)]
        pltpu.make_async_copy(view, view, ici_send.at[k]).wait()


def unload(v, o, sem):
    rows = o.shape[0] // PARTS
    copies = [
        pltpu.make_async_copy(v.at[pl.ds(rows * i, rows)], o.at[pl.ds(rows * i, rows)], sem.at[i]) for i in range(PARTS)
    ]
    for copy in copies:
        copy.start()
    for copy in copies:
        copy.wait()


def solution(mesh):
    def body(a, g):
        dma = pltpu.SemaphoreType.DMA
        held = pl.pallas_call(
            kernel,
            out_shape=pltpu.VMEM((2 * CHUNKS * UNIT, WIDE), BF16),
            in_specs=[pl.BlockSpec(memory_space=pltpu.HBM)] * 2,
            out_specs=pl.BlockSpec(memory_space=pltpu.VMEM),
            scratch_shapes=[
                pltpu.VMEM((2, 2048, 2 * UNIT), BF16),
                pltpu.VMEM((LOADS, 2048, TILE), BF16),
                pltpu.VMEM((CHUNKS * UNIT, WIDE), BF16),
                pltpu.VMEM((CHUNKS * UNIT, WIDE), F32),
                pltpu.VMEM((CHUNKS * SLOTS, WIDE), BF16),
                dma((2, 2)),
                dma((LOADS,)),
                dma((CHUNKS, 3)),
                dma((CHUNKS, 3)),
                dma((CHUNKS, 3, 20)),
                dma((3,)),
                dma,
                dma,
            ],
            compiler_params=pltpu.CompilerParams(
                collective_id=0, has_side_effects=True, vmem_limit_bytes=50_000_000
            ),
            name="sums",
        )(a, g)
        out = pl.pallas_call(
            unload,
            out_shape=jax.ShapeDtypeStruct(held.shape, held.dtype),
            in_specs=[pl.BlockSpec(memory_space=pltpu.VMEM)],
            out_specs=pl.BlockSpec(memory_space=pltpu.HBM),
            scratch_shapes=[dma((PARTS,))],
            compiler_params=pltpu.CompilerParams(vmem_limit_bytes=1 << 20),
            name="unload",
        )(held)
        return out.reshape(2, CHUNKS * UNIT, WIDE)

    spec = P(("rep", "dp"))
    return jax.shard_map(body, mesh=mesh, in_specs=(spec, spec), out_specs=P("rep"), check_vma=False)
```
